32 devices in a mesh: row: 4 (over y, core), col: 8 (over z, x).
Axes of the slice: x: 2, y: 2, z: 4, core: 2. Of those that a mesh axis runs over, the one named last changes fastest.
Arguments:
- eigvecs: float32 [1024, 50176], P('col', 'row'), may hold values from -6 to 6
- span_vectors: float32 [2, 32, 4, 128], P(None, 'row'), may hold values from -6 to 6
- span_offsets: int32 [2, 32], P(None, 'row'), may hold values from 0 to 12543, as said below
- panels: bfloat16 [2, 256, 50176], P(None, 'col', 'row'), may hold values from -0.026785714 to 0.026785714
Outputs:
- back_vectors: float32 [1024, 50176], P('col', 'row')
The draws below stay inside these ranges and needn't reach their ends.
Inputs may be any that keep to these rules, and one draw needn't show every extreme that they name: `span_offsets`: each block starts within the rows of its index of row and ends at most 128 rows after them, and inside the matrix; on every index of row but the last the last block of each sweep reaches into the next index's rows.
All inputs are finite; a program needn't handle non-finite values.
Results may differ from the reference program's by a relative error of at most 0.0075.
Values may be sent and summed in bfloat16 or wider, within the bound.
A program may use at most 128 MiB of HBM per device.

```python
import jax
import jax.numpy as jnp
from jax import lax

K = 1024
ROWS_DEV = 12544
N = 50176
BAND = 128
REFL = 4
SPANS_DEV = 8
SPANS = 32
SWEEPS = 2
WIDTH = 256
PANELS = 2
N_ROW = 4


def draw_span_offsets(key, part):
    key_base, key_last = jax.random.split(key, 2)
    offsets_all = jax.random.randint(key_base, (SWEEPS, N_ROW, SPANS_DEV), 0, ROWS_DEV - BAND + 1)
    last_span = jax.random.randint(key_last, (SWEEPS, N_ROW), ROWS_DEV - 3 * BAND // 4, ROWS_DEV - BAND // 4 + 1)
    device_ids = jnp.arange(N_ROW)[None, :]
    last_span = jnp.where(device_ids < N_ROW - 1, last_span, ROWS_DEV - BAND)
    offsets_all = offsets_all.at[:, :, SPANS_DEV - 1].set(last_span)
    return offsets_all.reshape(SWEEPS, N_ROW * SPANS_DEV).astype(jnp.int32)


def draw_panels(key, part):
    key_own = jax.random.fold_in(key, 17)
    own = jax.random.truncated_normal(key_own, -4.0, 4.0, (PANELS, WIDTH, N), jnp.float32)
    scaled = own * float(N) ** (-0.5)
    limit = 6.0 * float(N) ** (-0.5)
    return jnp.clip(scaled, -limit, limit).astype(jnp.bfloat16)


def levels(own_key, extent, cuts, least, high):
    def one(axis_at, shards_of):
        heights = jax.random.uniform(jax.random.fold_in(jax.random.fold_in(own_key, 6), axis_at), (shards_of,), jnp.float32, least / len(cuts), high / len(cuts))
        return jnp.repeat(jnp.exp(heights), extent[axis_at] // shards_of).reshape((-1,) + (1,) * (len(extent) - axis_at - 1))

    loudness = one(*cuts[0])
    for cut in cuts[1:]:
        loudness = loudness * one(*cut)
    return loudness


def centred(rng, shape, width, reach, cuts=(), held_as=jnp.bfloat16):
    factor_of = levels(rng, shape, cuts, -0.22, 0.18) if cuts else 1.0
    values = jax.random.normal(rng, shape, jnp.float32) * width * factor_of
    return jnp.minimum(jnp.maximum(values, -reach), reach).astype(held_as)


def setup_inputs(seed: int = 0) -> dict:
    streams_of = jax.random.split(jax.random.key(seed), 5)
    return {
        "eigvecs": centred(streams_of[0], (K, N), 1.0, 6.0, ((0, 8), (1, 4)), jnp.float32),
        "span_vectors": centred(streams_of[1], (SWEEPS, SPANS, REFL, BAND), 1.0, 6.0, ((1, 4),), jnp.float32),
        "span_offsets": draw_span_offsets(jax.random.fold_in(streams_of[4], 71), 0),
        "panels": draw_panels(jax.random.fold_in(streams_of[4], 71), 0),
    }


PRECISE = lax.Precision.HIGHEST
CONTRACT_LAST = (((1,), (1,)), ((), ()))
CONTRACT_FIRST = (((0,), (0,)), ((), ()))

def wy_matrix(gram_mat):
    return jnp.triu(gram_mat, 1) + 0.5 * jnp.diag(jnp.diag(gram_mat))

def apply_span(window, vectors):
    gram_mat = jnp.dot(vectors, vectors.T, precision=PRECISE)
    inner = jnp.dot(vectors, window.T, precision=PRECISE)
    coeffs = lax.linalg.triangular_solve(wy_matrix(gram_mat), inner, left_side=True, lower=False)
    return window - jnp.dot(coeffs.T, vectors, precision=PRECISE)

def reference(eigvecs, span_vectors, span_offsets, panels):
    eigen = eigvecs
    for sweep_at in range(SWEEPS):
        vectors = span_vectors[sweep_at]
        offsets = span_offsets[sweep_at]

        def advance(span_at, state, vectors=vectors, offsets=offsets):
            begin_at = (span_at // SPANS_DEV * ROWS_DEV + offsets[span_at]).astype(jnp.int32)
            window = lax.dynamic_slice_in_dim(state, begin_at, BAND, 1)
            return lax.dynamic_update_slice_in_dim(state, apply_span(window, vectors[span_at]), begin_at, 1)
        eigen = lax.fori_loop(0, SPANS, advance, eigen)
    for panel_at in range(PANELS):
        reflect = panels[panel_at]
        gram_mat = lax.dot_general(reflect.astype(jnp.float32), reflect.astype(jnp.float32), CONTRACT_LAST, preferred_element_type=jnp.float32)
        inner = lax.dot_general(reflect.astype(jnp.float32), eigen.astype(jnp.bfloat16).astype(jnp.float32), CONTRACT_LAST, preferred_element_type=jnp.float32)
        coeffs = lax.linalg.triangular_solve(wy_matrix(gram_mat), inner, left_side=True, lower=False)
        eigen = eigen - lax.dot_general(coeffs.astype(jnp.bfloat16).astype(jnp.float32), reflect.astype(jnp.float32), CONTRACT_FIRST, preferred_element_type=jnp.float32)
    return eigen
```

```python
import functools

import jax
import jax.numpy as jnp
from jax import lax
from jax.experimental import pallas as pl
from jax.experimental.pallas import tpu as pltpu
from jax.sharding import PartitionSpec as P

PRECISE = lax.Precision.HIGHEST
CONTRACT_LAST = (((1,), (1,)), ((), ()))
CONTRACT_FIRST = (((0,), (0,)), ((), ()))
LANES = 128


def shift_row(value, steps):
    count = lax.axis_size("row")
    first, last = (max(0, -steps), min(count, count - steps))
    return lax.ppermute(value, "row", [(source, source + steps) for source in range(first, last)])


def row_sum(value):
    count = lax.axis_size("row")
    if count & (count - 1):
        return lax.psum(value, "row")
    step = 1
    while step < count:
        value = value + lax.ppermute(value, "row", [(at, at ^ step) for at in range(count)])
        step *= 2
    return value


def spread_kernel(refl, offs_ref, vec_ref, out_ref):
    out_ref[...] = jnp.zeros_like(out_ref)
    spans = vec_ref.shape[0] // refl
    band = vec_ref.shape[1]
    wide = band + LANES
    per = 8 // refl
    for span_at in range(spans):
        group = span_at // per
        begin = offs_ref[span_at]
        base = pl.multiple_of(begin // LANES * LANES, LANES)
        rows = pl.ds(8 * group, 8)
        vectors = jnp.concatenate(
            [vec_ref[rows, :], jnp.zeros((8, LANES), jnp.float32)], axis=1
        )
        moved = pltpu.roll(vectors, begin - begin // LANES * LANES, 1)
        place = lax.broadcasted_iota(jnp.int32, (8, wide), 0) // refl
        out_ref[rows, pl.ds(base, wide)] += jnp.where(place == span_at % per, moved, 0.0)


def spread(vectors, offsets, refl, rows_dev):
    count, band = vectors.shape
    return pl.pallas_call(
        functools.partial(spread_kernel, refl),
        out_shape=jax.ShapeDtypeStruct((count, rows_dev + band), jnp.float32),
        in_specs=[
            pl.BlockSpec(memory_space=pltpu.SMEM),
            pl.BlockSpec(memory_space=pltpu.VMEM),
        ],
        out_specs=pl.BlockSpec(memory_space=pltpu.VMEM),
        cost_estimate=pl.CostEstimate(flops=0, bytes_accessed=8 * count * rows_dev, transcendentals=0),
    )(offsets, vectors)


def triangle_inverse(matrix):
    order = matrix.shape[0]
    row = lax.broadcasted_iota(jnp.int32, (order, order), 0)
    col = lax.broadcasted_iota(jnp.int32, (order, order), 1)
    diagonal = jnp.where(row == col, matrix, 0.0)
    down = 1.0 / jnp.sum(diagonal, axis=1, keepdims=True)
    across = 1.0 / jnp.sum(diagonal, axis=0, keepdims=True)
    inverse = jnp.where(row == col, down, 0.0)
    beside = (row // 2 == col // 2) & (row != col)
    inverse = inverse - jnp.where(beside, matrix * down * across, 0.0)
    size = 2
    while size < order:
        beside = (row // (2 * size) == col // (2 * size)) & (row // size != col // size)
        off = jnp.where(beside, matrix, 0.0)
        right = jnp.dot(off, inverse, precision=PRECISE, preferred_element_type=jnp.float32)
        inverse = inverse - jnp.dot(
            inverse, right, precision=PRECISE, preferred_element_type=jnp.float32
        )
        size *= 2
    return inverse


def solve_kernel(block, mat_ref, rhs_ref, out_ref):
    gram_mat = mat_ref[...]
    order = gram_mat.shape[0]
    row = lax.broadcasted_iota(jnp.int32, (order, order), 0)
    col = lax.broadcasted_iota(jnp.int32, (order, order), 1)
    before = (row // block > col // block) | ((row // block == col // block) & (row < col))
    matrix = jnp.where(before, gram_mat, jnp.where(row == col, 0.5 * gram_mat, 0.0))
    inverse = triangle_inverse(matrix)
    out_ref[...] = jnp.dot(
        inverse, rhs_ref[...], precision=PRECISE, preferred_element_type=jnp.float32
    ).astype(out_ref.dtype)


def solve(gram_mat, inner, block, dtype):
    order = gram_mat.shape[0]
    return pl.pallas_call(
        functools.partial(solve_kernel, block),
        out_shape=jax.ShapeDtypeStruct(inner.shape, dtype),
        in_specs=[pl.BlockSpec(memory_space=pltpu.VMEM)] * 2,
        out_specs=pl.BlockSpec(memory_space=pltpu.VMEM),
        cost_estimate=pl.CostEstimate(
            flops=200 * order**3, bytes_accessed=8 * order * order, transcendentals=0
        ),
    )(gram_mat, inner)


def sums_kernel(ref_ref, eig_ref, out_ref):
    width = ref_ref.shape[0]

    @pl.when(pl.program_id(0) == 0)
    def _():
        out_ref[...] = jnp.zeros_like(out_ref)

    reflect = ref_ref[...]
    out_ref[:, :width] += lax.dot_general(
        reflect, reflect, CONTRACT_LAST, preferred_element_type=jnp.float32
    )
    out_ref[:, width:] += lax.dot_general(
        reflect, eig_ref[...], CONTRACT_LAST, preferred_element_type=jnp.float32
    )


def tile_of(rows_dev, most):
    count = rows_dev // LANES
    return LANES * max(part for part in range(1, most + 1) if count % part == 0)


def local_sums(reflect, rounded):
    width, rows_dev = reflect.shape
    columns = rounded.shape[0]
    tile = tile_of(rows_dev, 14)
    return pl.pallas_call(
        sums_kernel,
        grid=(rows_dev // tile,),
        out_shape=jax.ShapeDtypeStruct((width, width + columns), jnp.float32),
        in_specs=[
            pl.BlockSpec((width, tile), lambda at: (0, at)),
            pl.BlockSpec((columns, tile), lambda at: (0, at)),
        ],
        out_specs=pl.BlockSpec((width, width + columns), lambda at: (0, 0)),
        cost_estimate=pl.CostEstimate(
            flops=2 * width * (width + columns) * rows_dev,
            bytes_accessed=2 * rows_dev * (width + columns),
            transcendentals=0,
        ),
    )(reflect, rounded)


def sweep_section(eigen, vectors, offsets):
    sweeps, spans_dev, refl, band = vectors.shape
    columns, rows_dev = eigen.shape
    rows = lax.axis_size("row")
    mine = lax.axis_index("row")
    own = spans_dev * refl
    count = sweeps * own
    spans = spread(vectors.reshape(count, band), offsets.reshape(-1), refl, rows_dev)
    tail = shift_row(spans[:, rows_dev:], 1)
    head = spans[:, :band]
    first = eigen[:, :band]
    inside = spans[:, :rows_dev]

    def times(left, right):
        return lax.dot_general(
            left, right, CONTRACT_LAST, precision=PRECISE, preferred_element_type=jnp.float32
        )

    packed = jnp.concatenate(
        [times(inside, eigen), times(tail, first), times(spans, spans), times(head, tail)], axis=1
    )
    packed = lax.all_gather(packed, "row", axis=0, tiled=False)
    inner = packed[:, :, :columns]
    above = packed[:, :, columns : 2 * columns]
    inner = inner + jnp.concatenate([above[1:], jnp.zeros_like(above[:1])], axis=0)
    shape = (rows, sweeps, own, sweeps, own)
    gram_own = packed[:, :, 2 * columns : 2 * columns + count].reshape(shape)
    gram_prev = packed[:, :, 2 * columns + count :].reshape(shape)
    same = jnp.eye(rows, dtype=jnp.float32)[:, :, None, None, None, None]
    back = jnp.eye(rows, k=-1, dtype=jnp.float32)[:, :, None, None, None, None]
    prev = gram_prev.transpose(0, 3, 4, 1, 2)
    full = same * gram_own[:, None] + back * gram_prev[:, None]
    full = full + back.transpose(1, 0, 2, 3, 4, 5) * prev[None]
    total = rows * count
    full = full.transpose(2, 0, 3, 4, 1, 5).reshape(total, total)
    inner = inner.reshape(rows, sweeps, own, columns).transpose(1, 0, 2, 3).reshape(total, columns)
    coeffs = solve(full, inner, refl, jnp.float32)
    coeffs = coeffs.reshape(sweeps, rows, own, columns)

    def of_row(place):
        return lax.dynamic_index_in_dim(coeffs, place, 1, keepdims=False).reshape(count, columns)

    own_part = of_row(mine)
    prev_part = of_row(jnp.maximum(mine - 1, 0))
    updated = eigen - lax.dot_general(
        own_part, inside, CONTRACT_FIRST, precision=PRECISE, preferred_element_type=jnp.float32
    )
    begin = updated[:, :band] - lax.dot_general(
        prev_part, tail, CONTRACT_FIRST, precision=PRECISE, preferred_element_type=jnp.float32
    )
    return lax.dynamic_update_slice_in_dim(updated, begin, 0, 1)


def local(eigvecs, span_vectors, span_offsets, panels):
    reflectors = [
        lax.all_gather(panels[panel_at], "col", axis=0, tiled=True)
        for panel_at in range(panels.shape[0])
    ]
    eigen = sweep_section(eigvecs, span_vectors, span_offsets)
    for reflect in reflectors:
        width = reflect.shape[0]
        both = row_sum(local_sums(reflect, eigen.astype(jnp.bfloat16)))
        coeffs = solve(both[:, :width], both[:, width:], width, jnp.bfloat16)
        eigen = eigen - lax.dot_general(
            coeffs, reflect, CONTRACT_FIRST, preferred_element_type=jnp.float32
        )
    return eigen


def solution(mesh):
    return jax.shard_map(
        local,
        mesh=mesh,
        in_specs=(
            P("col", "row"),
            P(None, "row", None, None),
            P(None, "row"),
            P(None, "col", "row"),
        ),
        out_specs=P("col", "row"),
        check_vma=False,
    )
```

```python
import functools

import jax
import jax.numpy as jnp
from jax import lax
from jax.experimental import pallas as pl
from jax.experimental.pallas import tpu as pltpu
from jax.sharding import PartitionSpec as P

PRECISE = lax.Precision.HIGHEST
CONTRACT_LAST = (((1,), (1,)), ((), ()))
CONTRACT_FIRST = (((0,), (0,)), ((), ()))
LANES = 128


def shift_row(value, steps):
    count = lax.axis_size("row")
    first, last = (max(0, -steps), min(count, count - steps))
    return lax.ppermute(value, "row", [(source, source + steps) for source in range(first, last)])


def row_sum(value):
    count = lax.axis_size("row")
    if count & (count - 1):
        return lax.psum(value, "row")
    step = 1
    while step < count:
        value = value + lax.ppermute(value, "row", [(at, at ^ step) for at in range(count)])
        step *= 2
    return value


def spread_kernel(refl, offs_ref, vec_ref, out_ref):
    out_ref[...] = jnp.zeros_like(out_ref)
    spans = vec_ref.shape[0] // refl
    band = vec_ref.shape[1]
    wide = band + LANES
    per = 8 // refl
    for span_at in range(spans):
        group = span_at // per
        begin = offs_ref[span_at]
        base = pl.multiple_of(begin // LANES * LANES, LANES)
        rows = pl.ds(8 * group, 8)
        vectors = jnp.concatenate(
            [vec_ref[rows, :], jnp.zeros((8, LANES), jnp.float32)], axis=1
        )
        moved = pltpu.roll(vectors, begin - begin // LANES * LANES, 1)
        place = lax.broadcasted_iota(jnp.int32, (8, wide), 0) // refl
        out_ref[rows, pl.ds(base, wide)] += jnp.where(place == span_at % per, moved, 0.0)


def spread(vectors, offsets, refl, rows_dev):
    count, band = vectors.shape
    return pl.pallas_call(
        functools.partial(spread_kernel, refl),
        out_shape=jax.ShapeDtypeStruct((count, rows_dev + band), jnp.float32),
        in_specs=[
            pl.BlockSpec(memory_space=pltpu.SMEM),
            pl.BlockSpec(memory_space=pltpu.VMEM),
        ],
        out_specs=pl.BlockSpec(memory_space=pltpu.VMEM),
        cost_estimate=pl.CostEstimate(flops=0, bytes_accessed=8 * count * rows_dev, transcendentals=0),
    )(offsets, vectors)


def triangle_inverse(matrix, down_at, across_at):
    order = matrix.shape[0]
    same = down_at == across_at
    diagonal = jnp.where(same, matrix, 0.0)
    down = 1.0 / jnp.sum(diagonal, axis=1, keepdims=True)
    across = 1.0 / jnp.sum(diagonal, axis=0, keepdims=True)
    inverse = jnp.where(same, down, 0.0)
    beside = (down_at // 2 == across_at // 2) & (down_at != across_at)
    inverse = inverse - jnp.where(beside, matrix * down * across, 0.0)
    size = 2
    while size < order:
        together = down_at // (2 * size) == across_at // (2 * size)
        beside = together & (down_at // size != across_at // size)
        off = jnp.where(beside, matrix, 0.0)
        right = jnp.dot(off, inverse, precision=PRECISE, preferred_element_type=jnp.float32)
        inverse = inverse - jnp.dot(
            inverse, right, precision=PRECISE, preferred_element_type=jnp.float32
        )
        size *= 2
    return inverse


def solve_kernel(block, places_ref, mat_ref, rhs_ref, out_ref):
    gram_mat = mat_ref[...]
    order = gram_mat.shape[0]
    pieces = places_ref.shape[0]
    piece = order // pieces
    true_at = []
    for axis in range(2):
        at = lax.broadcasted_iota(jnp.int32, (order, order), axis)
        part = at // piece
        moved = at - part * piece
        for index in range(pieces):
            moved = moved + jnp.where(part == index, places_ref[index] * piece, 0)
        true_at.append(moved)
    row, col = true_at
    before = (row // block > col // block) | ((row // block == col // block) & (row < col))
    matrix = jnp.where(before, gram_mat, jnp.where(row == col, 0.5 * gram_mat, 0.0))
    inverse = triangle_inverse(matrix, row, col)
    out_ref[...] = jnp.dot(
        inverse, rhs_ref[...], precision=PRECISE, preferred_element_type=jnp.float32
    ).astype(out_ref.dtype)


def solve(places, gram_mat, inner, block, dtype):
    order = gram_mat.shape[0]
    return pl.pallas_call(
        functools.partial(solve_kernel, block),
        out_shape=jax.ShapeDtypeStruct(inner.shape, dtype),
        in_specs=[pl.BlockSpec(memory_space=pltpu.SMEM)]
        + [pl.BlockSpec(memory_space=pltpu.VMEM)] * 2,
        out_specs=pl.BlockSpec(memory_space=pltpu.VMEM),
        cost_estimate=pl.CostEstimate(
            flops=500 * order**3, bytes_accessed=8 * order * order, transcendentals=0
        ),
    )(places, gram_mat, inner)


def sums_kernel(eig_ref, *refs):
    out_ref = refs[-1]
    width = out_ref.shape[0]

    @pl.when(pl.program_id(0) == 0)
    def _():
        out_ref[...] = jnp.zeros_like(out_ref)

    reflect = jnp.concatenate([ref[...] for ref in refs[:-1]], axis=0)
    out_ref[:, :width] += lax.dot_general(
        reflect, reflect, CONTRACT_LAST, preferred_element_type=jnp.float32
    )
    out_ref[:, width:] += lax.dot_general(
        reflect, eig_ref[...], CONTRACT_LAST, preferred_element_type=jnp.float32
    )


def tile_of(rows_dev, most):
    count = rows_dev // LANES
    return LANES * max(part for part in range(1, most + 1) if count % part == 0)


def local_sums(blocks, rounded):
    columns, rows_dev = rounded.shape
    width = sum(block.shape[0] for block in blocks)
    tile = tile_of(rows_dev, 14)
    return pl.pallas_call(
        sums_kernel,
        grid=(rows_dev // tile,),
        out_shape=jax.ShapeDtypeStruct((width, width + columns), jnp.float32),
        in_specs=[
            pl.BlockSpec((value.shape[0], tile), lambda at: (0, at))
            for value in (rounded, *blocks)
        ],
        out_specs=pl.BlockSpec((width, width + columns), lambda at: (0, 0)),
        cost_estimate=pl.CostEstimate(
            flops=6 * width * (width + columns) * rows_dev,
            bytes_accessed=2 * rows_dev * (width + columns),
            transcendentals=0,
        ),
    )(rounded, *blocks)


def update_kernel(count, eig_ref, coef_ref, *refs):
    reflect = jnp.concatenate([ref[...] for ref in refs[:count]], axis=0)
    value = eig_ref[...] - lax.dot_general(
        coef_ref[...], reflect, CONTRACT_FIRST, preferred_element_type=jnp.float32
    )
    for out_ref in refs[count:]:
        out_ref[...] = value.astype(out_ref.dtype)


def panel_update(eigen, coeffs, blocks, types):
    columns, rows_dev = eigen.shape
    width = coeffs.shape[0]
    tile = tile_of(rows_dev, 14)
    return pl.pallas_call(
        functools.partial(update_kernel, len(blocks)),
        grid=(rows_dev // tile,),
        out_shape=[jax.ShapeDtypeStruct(eigen.shape, dtype) for dtype in types],
        in_specs=[
            pl.BlockSpec((columns, tile), lambda at: (0, at)),
            pl.BlockSpec((width, columns), lambda at: (0, 0)),
        ]
        + [pl.BlockSpec((block.shape[0], tile), lambda at: (0, at)) for block in blocks],
        out_specs=[pl.BlockSpec((columns, tile), lambda at: (0, at)) for _ in types],
        cost_estimate=pl.CostEstimate(
            flops=2 * width * columns * rows_dev,
            bytes_accessed=rows_dev * (2 * width + 12 * columns),
            transcendentals=0,
        ),
    )(eigen, coeffs, *blocks)


def folded_ring(count):
    return [0] + list(range(1, count, 2)) + list(range(2, count, 2))[::-1]


def gather_blocks(own):
    count = lax.axis_size("col")
    ring = folded_ring(count // 2)
    size = len(ring)
    onward = [
        (2 * ring[at] + side, 2 * ring[(at + 1) % size] + side)
        for at in range(size)
        for side in range(2)
    ]
    across = [(at, at ^ 1) for at in range(count)]
    near, far = [own], []
    for step in range(size):
        far.append(lax.ppermute(near[-1], "col", across))
        if step < size - 1:
            near.append(lax.ppermute(near[-1], "col", onward))
    return near + far


def block_places():
    count = lax.axis_size("col")
    ring = folded_ring(count // 2)
    size = len(ring)
    table = []
    for at in range(count):
        before = [ring[(ring.index(at // 2) - step) % size] for step in range(size)]
        table.append([2 * row + at % 2 for row in before] + [2 * row + 1 - at % 2 for row in before])
    return lax.dynamic_index_in_dim(
        jnp.array(table, jnp.int32), lax.axis_index("col"), 0, keepdims=False
    )


def sweep_section(eigen, vectors, offsets):
    sweeps, spans_dev, refl, band = vectors.shape
    columns, rows_dev = eigen.shape
    rows = lax.axis_size("row")
    mine = lax.axis_index("row")
    own = spans_dev * refl
    count = sweeps * own
    spans = spread(vectors.reshape(count, band), offsets.reshape(-1), refl, rows_dev)
    tail = shift_row(spans[:, rows_dev:], 1)
    head = spans[:, :band]
    first = eigen[:, :band]
    inside = spans[:, :rows_dev]

    def times(left, right):
        return lax.dot_general(
            left, right, CONTRACT_LAST, precision=PRECISE, preferred_element_type=jnp.float32
        )

    packed = jnp.concatenate(
        [times(inside, eigen), times(tail, first), times(spans, spans), times(head, tail)], axis=1
    )
    packed = lax.all_gather(packed, "row", axis=0, tiled=False)
    inner = packed[:, :, :columns]
    above = packed[:, :, columns : 2 * columns]
    inner = inner + jnp.concatenate([above[1:], jnp.zeros_like(above[:1])], axis=0)
    shape = (rows, sweeps, own, sweeps, own)
    gram_own = packed[:, :, 2 * columns : 2 * columns + count].reshape(shape)
    gram_prev = packed[:, :, 2 * columns + count :].reshape(shape)
    same = jnp.eye(rows, dtype=jnp.float32)[:, :, None, None, None, None]
    back = jnp.eye(rows, k=-1, dtype=jnp.float32)[:, :, None, None, None, None]
    prev = gram_prev.transpose(0, 3, 4, 1, 2)
    full = same * gram_own[:, None] + back * gram_prev[:, None]
    full = full + back.transpose(1, 0, 2, 3, 4, 5) * prev[None]
    total = rows * count
    full = full.transpose(2, 0, 3, 4, 1, 5).reshape(total, total)
    inner = inner.reshape(rows, sweeps, own, columns).transpose(1, 0, 2, 3).reshape(total, columns)
    coeffs = solve(jnp.zeros((1,), jnp.int32), full, inner, refl, jnp.float32)
    coeffs = coeffs.reshape(sweeps, rows, own, columns)

    def of_row(place):
        return lax.dynamic_index_in_dim(coeffs, place, 1, keepdims=False).reshape(count, columns)

    own_part = of_row(mine)
    prev_part = of_row(jnp.maximum(mine - 1, 0))
    updated = eigen - lax.dot_general(
        own_part, inside, CONTRACT_FIRST, precision=PRECISE, preferred_element_type=jnp.float32
    )
    begin = updated[:, :band] - lax.dot_general(
        prev_part, tail, CONTRACT_FIRST, precision=PRECISE, preferred_element_type=jnp.float32
    )
    return lax.dynamic_update_slice_in_dim(updated, begin, 0, 1)


def local(eigvecs, span_vectors, span_offsets, panels):
    count = panels.shape[0]
    gathered = [gather_blocks(panels[panel_at]) for panel_at in range(count)]
    places = block_places()
    eigen = sweep_section(eigvecs, span_vectors, span_offsets)
    rounded = eigen.astype(jnp.bfloat16)
    for panel_at, blocks in enumerate(gathered):
        both = row_sum(local_sums(blocks, rounded))
        width = both.shape[0]
        coeffs = solve(places, both[:, :width], both[:, width:], width, jnp.bfloat16)
        if panel_at < count - 1:
            eigen, rounded = panel_update(eigen, coeffs, blocks, (jnp.float32, jnp.bfloat16))
        else:
            (eigen,) = panel_update(eigen, coeffs, blocks, (jnp.float32,))
    return eigen


def solution(mesh):
    return jax.shard_map(
        local,
        mesh=mesh,
        in_specs=(
            P("col", "row"),
            P(None, "row", None, None),
            P(None, "row"),
            P(None, "col", "row"),
        ),
        out_specs=P("col", "row"),
        check_vma=False,
    )
```
